128 devices in a mesh: bank: 4 (over y), zero: 32 (over z, x, core).
Axes of the slice: x: 4, y: 4, z: 4, core: 2. Of those that a mesh axis runs over, the one named last changes fastest.
Arguments:
- master_gate: float32 [64, 2048, 1408], P('bank', 'zero'), may hold values from -0.25 to 0.25
- master_up: float32 [64, 2048, 1408], P('bank', 'zero'), may hold values from -0.25 to 0.25
- master_down: float32 [64, 1408, 2048], P('bank', None, 'zero'), may hold values from -0.3125 to 0.3125
- router_weight: float32 [2048, 64], P('zero', 'bank'), may hold values from -0.125 to 0.125
- router_gain: float32 [2048], P('zero'), may hold values from 0.25 to 1.75
Outputs:
- final_gate: bfloat16 [64, 2048, 1408], P('bank', None, 'zero')
- final_up: bfloat16 [64, 2048, 1408], P('bank', None, 'zero')
- final_down: bfloat16 [64, 1408, 2048], P('bank', 'zero')
- scale_gate: float32 [64, 1408], P('bank', 'zero')
- scale_up: float32 [64, 1408], P('bank', 'zero')
- scale_down: float32 [64, 1408], P('bank', 'zero')
- serve_router: bfloat16 [2048, 64], replicated
The draws below stay inside these ranges and needn't reach their ends.
All inputs are finite; a program needn't handle non-finite values. Where the reference program divides by a largest or mean magnitude, that divisor is 1e-20 or more.
Results may differ from the reference program's by a relative error of at most 0.001.
Values may be sent and summed in bfloat16 or wider, within the bound.
No kernel may reach another device: no remote copies, remote signals or barrier semaphores. Data moves between devices by JAX's collectives and lax.ppermute only.
A program may use at most 128 MiB of HBM per device.

```python
import jax
import jax.numpy as jnp

EXPERTS = 64
D_MODEL = 2048
D_EXPERT = 1408


def strengthened(array, rng, source, target, parts, factor):
    def block_of(dim):
        return (jnp.arange(array.shape[dim]) // (array.shape[dim] // parts)).reshape((-1,) + (1,) * (array.ndim - 1 - dim))

    one_side = jax.random.permutation(rng, parts)[block_of(target)]
    second = (block_of(target) + parts // 2) % parts
    return jnp.where((block_of(source) == one_side) | (block_of(source) == second), factor * array, array)


def level_of(stream_key, extent, pieces, least, top_value):
    def one(axis_at, parts):
        heights = jax.random.uniform(jax.random.fold_in(jax.random.fold_in(stream_key, 6), axis_at), (parts,), jnp.float32, least / len(pieces), top_value / len(pieces))
        return jnp.repeat(jnp.exp(heights), extent[axis_at] // parts).reshape((-1,) + (1,) * (len(extent) - axis_at - 1))

    level = one(*pieces[0])
    for cut in pieces[1:]:
        level = level * one(*cut)
    return level


def bell_draw(rng, shape, spread, most, pieces=(), dtype=jnp.bfloat16):
    loudness = level_of(rng, shape, pieces, -0.22, 0.18) if pieces else 1.0
    result = jax.random.normal(rng, shape, jnp.float32) * spread * loudness
    return jnp.minimum(jnp.maximum(result, -most), most).astype(dtype)


def noise_with(own_key, extent, spread, most, cuts, heavy, dtype=jnp.bfloat16):
    result = spread * jax.random.normal(own_key, extent, jnp.float32)
    if cuts:
        result = result * level_of(own_key, extent, cuts, -0.22, 0.18)
    return jnp.clip(strengthened(result, jax.random.fold_in(own_key, 3), *heavy), -most, most).astype(dtype)


def setup_inputs(seed: int = 0) -> dict:
    keys = jax.random.split(jax.random.key(seed), 6)
    return {
        "master_gate": noise_with(keys[0], (EXPERTS, D_MODEL, D_EXPERT), D_MODEL ** -0.5, 0.25, ((0, 4), (1, 32)), (1, 2, 32, 2.75), jnp.float32),
        "master_up": noise_with(keys[1], (EXPERTS, D_MODEL, D_EXPERT), D_MODEL ** -0.5, 0.25, ((0, 4), (1, 32)), (1, 2, 32, 2.75), jnp.float32),
        "master_down": noise_with(keys[2], (EXPERTS, D_EXPERT, D_MODEL), D_EXPERT ** -0.5, 0.3125, ((0, 4), (2, 32)), (2, 1, 32, 2.75), jnp.float32),
        "router_weight": bell_draw(keys[3], (D_MODEL, EXPERTS), D_MODEL ** -0.5, 0.125, ((0, 32), (1, 4)), jnp.float32),
        "router_gain": jnp.clip(1.0 + 0.15 * jax.random.normal(keys[4], (D_MODEL,), jnp.float32), 0.25, 1.75),
    }


def reference(master_gate, master_up, master_down, router_weight, router_gain):
    scale_gate = jnp.max(jnp.abs(master_gate), axis=1)
    final_gate = (master_gate / jnp.expand_dims(scale_gate, 1)).astype(jnp.bfloat16)
    scale_up = jnp.max(jnp.abs(master_up), axis=1)
    final_up = (master_up / jnp.expand_dims(scale_up, 1)).astype(jnp.bfloat16)
    scale_down = jnp.max(jnp.abs(master_down), axis=2)
    final_down = (master_down / jnp.expand_dims(scale_down, 2)).astype(jnp.bfloat16)
    serve_router = (router_weight * router_gain[:, None]).astype(jnp.bfloat16)
    return final_gate, final_up, final_down, scale_gate, scale_up, scale_down, serve_router
```

```python
import functools

import jax
import jax.numpy as jnp
from jax import lax
from jax.experimental import pallas as pl
from jax.experimental.pallas import tpu as pltpu
from jax.sharding import Mesh
from jax.sharding import PartitionSpec as P

ZERO = ("zero_0", "zero_1", "zero_2")
PAIRS_A = [(0, 1), (1, 0), (2, 3), (3, 2)]
PAIRS_B = [(1, 2), (2, 1), (3, 0), (0, 3)]
ROUNDS = (
    ("zero_2", [(0, 1), (1, 0)]),
    ("zero_1", PAIRS_A),
    ("zero_1", PAIRS_B),
    ("zero_0", PAIRS_A),
    ("zero_0", PAIRS_B),
)
LANES = 128


def max_over_zero(part):
    for axis, pairs in ROUNDS:
        part = jnp.maximum(part, lax.ppermute(part, axis, pairs))
    return part


def pack_kernel(n_in, *refs):
    xs, ss, (out, turned) = refs[:n_in], refs[n_in : 2 * n_in], refs[2 * n_in :]
    for a in range(n_in):
        recip = 1.0 / ss[a][...]
        for low in range(8):
            both = jnp.concatenate(
                [xs[a][low] * recip[low : low + 1], xs[a][low + 8] * recip[low + 8 : low + 9]], axis=0
            )
            turned[pl.ds(low, LANES, stride=8), :] = both.T
        out[a] = turned[...].astype(jnp.bfloat16)


def pack(xs, scales):
    n_in = len(xs)
    e, k, n = xs[0].shape
    return pl.pallas_call(
        functools.partial(pack_kernel, n_in),
        grid=(n // LANES,),
        in_specs=[pl.BlockSpec((e, k, LANES), lambda j: (0, 0, j))] * n_in
        + [pl.BlockSpec((e, LANES), lambda j: (0, j))] * n_in,
        out_specs=pl.BlockSpec((n_in, LANES * 8, LANES), lambda j: (0, j, 0)),
        out_shape=jax.ShapeDtypeStruct((n_in, n * 8, LANES), jnp.bfloat16),
        scratch_shapes=[pltpu.VMEM((LANES * 8, LANES), jnp.float32)],
        cost_estimate=pl.CostEstimate(flops=n_in * 20_000_000, bytes_accessed=n_in * 9_000_000, transcendentals=0),
        name=f"pack{n_in}",
    )(*xs, *scales)


def unpack_kernel(pieces, got, out):
    half = LANES // 2
    for c in range(pieces // 2):
        even, odd = got[2 * c], got[2 * c + 1]
        cols = pl.ds(c * LANES, LANES)
        out[:, 0:8, cols] = jnp.concatenate([even[:, :, :half], odd[:, :, :half]], axis=2)
        out[:, 8:16, cols] = jnp.concatenate([even[:, :, half:], odd[:, :, half:]], axis=2)


def unpack(got, first, count, step):
    pieces = got.shape[0]
    return pl.pallas_call(
        functools.partial(unpack_kernel, pieces),
        grid=(count // step,),
        in_specs=[pl.BlockSpec((pieces, step, 8, LANES), lambda j: (0, first // step + j, 0, 0))],
        out_specs=pl.BlockSpec((step, 16, pieces * 64), lambda j: (j, 0, 0)),
        out_shape=jax.ShapeDtypeStruct((count, 16, pieces * 64), jnp.bfloat16),
        cost_estimate=pl.CostEstimate(flops=3_000_000, bytes_accessed=6_000_000, transcendentals=0),
        name=f"unpack{first}",
    )(got)


def shards(master_gate, master_up, master_down, router_weight, router_gain):
    zeros = lax.axis_size(ZERO)
    gate, up, down = master_gate, master_up, jnp.swapaxes(master_down, 1, 2)
    cols = gate.shape[2] // zeros

    def local_max(x):
        return jnp.max(jnp.abs(x), axis=1)

    piece = (router_weight * router_gain[:, None]).astype(jnp.bfloat16).T
    piece = jnp.concatenate([piece[:8], piece[8:]], axis=1)

    scale_gate = max_over_zero(local_max(gate))
    packed = pack([gate], [scale_gate]).reshape(zeros, cols, 8, LANES)
    rest, packed = lax.optimization_barrier((jnp.stack([local_max(up), local_max(down)]), packed))
    packed = jnp.concatenate([packed, jnp.broadcast_to(piece, (zeros, 1, 8, LANES))], axis=1)
    got1 = lax.all_to_all(packed, ZERO, 0, 0, tiled=True)

    scale_up, scale_down = max_over_zero(rest)
    packed = pack([up, down], [scale_up, scale_down]).reshape(2, zeros, cols, 8, LANES)
    packed = jnp.swapaxes(packed, 0, 1).reshape(zeros, 2 * cols, 8, LANES)
    got2 = lax.all_to_all(packed, ZERO, 0, 0, tiled=True)

    final_gate = unpack(got1, 0, cols, 4)
    rows = unpack(got1, cols, 1, 1)[0]
    final_up = unpack(got2, 0, cols, 4)
    final_down = unpack(got2, cols, cols, 4)

    serve = lax.all_gather(rows, "bank").reshape(-1, rows.shape[1]).T
    here = lax.axis_index(ZERO) * cols
    scales = [lax.dynamic_slice_in_dim(s, here, cols, axis=1) for s in (scale_gate, scale_up, scale_down)]
    return (
        jnp.transpose(final_gate, (1, 2, 0)),
        jnp.transpose(final_up, (1, 2, 0)),
        jnp.transpose(final_down, (1, 0, 2)),
        *scales,
        serve,
    )


def solution(mesh):
    torus = Mesh(
        mesh.devices.reshape(mesh.shape["bank"], 4, 4, 2), ("bank", "zero_0", "zero_1", "zero_2")
    )
    placed = (
        P("bank", ZERO, None),
        P("bank", ZERO, None),
        P("bank", None, ZERO),
        P(ZERO, "bank"),
        P(ZERO),
    )
    return jax.shard_map(
        shards,
        mesh=torus,
        in_specs=placed,
        out_specs=(
            P("bank", None, ZERO),
            P("bank", None, ZERO),
            P("bank", ZERO, None),
            P("bank", ZERO),
            P("bank", ZERO),
            P("bank", ZERO),
            P(),
        ),
        check_vma=False,
    )
```
